256 devices in a mesh: groups: 2 (over z), attn: 16 (over y, core), expert: 8 (over x).
Axes of the slice: x: 8, y: 8, z: 2, core: 2. Of those that a mesh axis runs over, the one named last changes fastest.
The devices are a block of a 8x8x16 slice.
Arguments:
- tokens: bfloat16 [4096, 4096], P(('groups', 'attn'), 'expert'), parts along dimension 0, may hold values from -6 to 6
- expert_ids: int32 [4096, 8], P(('groups', 'attn')), parts along dimension 0, may hold values from 0 to 63, all different within a row; in each aligned block of 128 rows (0 to 127, 128 to 255, ...) at most 48 rows name the same one
- gate_weight: bfloat16 [4096, 8], P(('groups', 'attn')), parts along dimension 0, may hold values from 0.049804688 to 0.29882812
- w_gate: bfloat16 [64, 4096, 768], P('attn', 'expert'), may hold values from -0.09375 to 0.09375
- w_up: bfloat16 [64, 4096, 768], P('attn', 'expert'), may hold values from -0.09375 to 0.09375
- w_down: bfloat16 [64, 768, 4096], P('attn', None, 'expert'), may hold values from -0.21875 to 0.21875
- query: bfloat16 [512, 64, 128], P(('groups', 'attn', 'expert')), parts along dimension 0, may hold values from -100 to 100
- cache_k: bfloat16 [512, 768, 4, 128], P(('groups', 'attn', 'expert')), parts along dimension 0, may hold values from -6 to 6
- cache_v: bfloat16 [512, 768, 4, 128], P(('groups', 'attn', 'expert')), parts along dimension 0, may hold values from -6 to 6
- lengths: int32 [512], P(('groups', 'attn', 'expert')), parts along dimension 0, may hold values from 2 to 768, as said below
Outputs:
- moe_out: bfloat16 [4096, 4096], P(('groups', 'attn'), 'expert'), parts along dimension 0
- attn_out: bfloat16 [512, 8192], P(('groups', 'attn', 'expert')), parts along dimension 0
The draws below stay inside these ranges and needn't reach their ends.
There are 2 independent parts, one for each index of `groups`. The reference program is written for one: setup_inputs(seed, part) draws one part's arguments, and reference() takes and returns one part's arrays. A program takes and returns all parts, laid end to end along the dimension named above; an argument that names none is the same for every part. Nothing has to cross between parts.
Inputs may be any that keep to these rules, and one draw needn't show every extreme that they name: `expert_ids`: each row names 8 different experts. In the rows of one index of attn (aligned blocks of 128 rows) no expert is named by more than 48 rows, and in some block some expert by exactly 48. `lengths`: some sequence has all 768 positions live.
All inputs are finite; a program needn't handle non-finite values.
Results may differ from the reference program's by a relative error of at most 0.025.
Values may be sent and summed in bfloat16 or wider, within the bound.
A program may use at most 64 MiB of HBM per device.

```python
import math
import jax
import jax.numpy as jnp
import numpy as np
from jax import lax

D = 4096
FF = 768
TOPK = 8
TOK_DEV = 128
Q_HEADS = 64
KV_HEADS = 4
HEAD_DIM = 128
CTX = 768
EXPERTS = 64
TOKENS = 2048
SEQS = 256
FEAT_DEV = 512
CAPACITY = 256
SLOT = 48
N_EXPERT = 8


def attention_inputs(key):
    keys_key = jax.random.fold_in(key, 101)
    query_key = jax.random.fold_in(key, 102)
    shape_keys = (SEQS, CTX, KV_HEADS, HEAD_DIM)
    shape_query = (SEQS, Q_HEADS, HEAD_DIM)
    key_rows = jnp.clip(jax.random.normal(keys_key, shape_keys, jnp.float32), -6.0, 6.0)
    query_rows = jnp.clip(jax.random.normal(query_key, shape_query, jnp.float32), -6.0, 6.0)
    return (key_rows, query_rows)


def draw_query(key, part):
    return attention_inputs(key)[1].astype(jnp.bfloat16)


def draw_cache_k(key, part):
    return attention_inputs(key)[0].astype(jnp.bfloat16)


def draw_lengths(key, part):
    base_lengths = jax.random.randint(jax.random.fold_in(key, 201), (SEQS,), 2, CTX + 1, dtype=jnp.int32)
    full_index = jax.random.randint(jax.random.fold_in(key, 202), (), 0, SEQS, dtype=jnp.int32)
    return jnp.where(jnp.arange(SEQS, dtype=jnp.int32) == full_index, CTX, base_lengths).astype(jnp.int32)


def block_scale(own_key, shape, cuts, smallest, top_value):
    factor_of = 1.0
    for axis_at, shards_of in cuts:
        steps = jax.random.uniform(jax.random.fold_in(jax.random.fold_in(own_key, 6), axis_at), (shards_of,), jnp.float32, smallest / len(cuts), top_value / len(cuts))
        factor_of = factor_of * jnp.repeat(jnp.exp(steps), shape[axis_at] // shards_of).reshape((-1,) + (1,) * (len(shape) - 1 - axis_at))
    return factor_of


def deal_out(stream_key, own, number, rows, count, top, most, slope):
    order = jax.random.permutation(stream_key, count)
    crowded, ordinary = shares(count, rows * top, most, slope, True), shares(count, rows * top, most, slope, False)
    places = jnp.arange(count)

    def named(sizes, offset_by):
        used = int((sizes > 0).sum())
        fixed = max(1, used // 4)
        passed = fixed + (places - fixed + offset_by * (used - fixed)) % max(1, count - fixed)
        return jnp.zeros((count,), jnp.int32).at[order[jnp.where(places < fixed, places, passed)]].set(jnp.asarray(sizes, jnp.int32))

    sizes = jnp.where(number % 4 == 0, named(crowded, number // 4), named(ordinary, number - number // 4 - 1))
    mixed = jax.random.permutation(jax.random.fold_in(own, 3), count)
    donor, taker = mixed[0:count // 2 * 2:2], mixed[1:count // 2 * 2:2]
    margin = jnp.minimum(sizes[donor] - 1, most - sizes[taker]) // 2
    margin = jnp.where((donor == order[0]) | (taker == order[0]) | (sizes[taker] == 0), 0, jnp.maximum(margin, 0))
    passed = jax.random.randint(jax.random.fold_in(own, 4), (count // 2,), 0, 1 << 20) % (margin + 1)
    sizes = sizes.at[donor].add(-passed).at[taker].add(passed)
    items = jnp.searchsorted(jnp.cumsum(sizes), jnp.arange(rows * top), side="right").astype(jnp.int32)
    table = items.reshape(top, rows).T
    table = table[jax.random.permutation(jax.random.fold_in(own, 1), rows)]
    offset_by = jax.random.randint(jax.random.fold_in(own, 2), (rows, 1), 0, top)
    return jnp.take_along_axis(table, (jnp.arange(top)[None, :] + offset_by) % top, axis=1)


def shares(number_of, total, reach, slope, full):
    portions = [(1 << 20) // math.isqrt(rank ** slope) + 1 for rank in range(1, number_of + 1)]
    largest = reach if full else min(reach, max(-(-total // number_of), total * portions[0] // sum(portions)))
    least = 1 if total - largest >= number_of - 1 else 0
    given, rest = [largest] + [least] * (number_of - 1), total - largest - least * (number_of - 1)
    while rest > 0:
        movable = [i for i in range(1, number_of) if given[i] < largest] or [i for i in range(1, number_of) if given[i] < reach]
        mass, remaining = sum([portions[i] for i in movable]), rest
        for i in movable:
            addition = min(reach - given[i], max(1, remaining * portions[i] // mass), rest)
            given[i] = given[i] + addition
            rest = rest - addition
    return np.array(given)


def centred(rng, extent, scale, reach, split=(), held_as=jnp.bfloat16):
    values = scale * jax.random.normal(rng, extent, jnp.float32)
    if split:
        values = values * block_scale(rng, extent, split, -0.22, 0.18)
    return jnp.clip(values, -reach, reach).astype(held_as)


def setup_inputs(seed: int = 0, part: int = 0) -> dict:
    keys = jax.random.split(jax.random.key(seed), 11)
    own_keys = jax.random.split(jax.random.fold_in(keys[10], part), 11)
    tokens = centred(own_keys[0], (TOKENS, D), 1.0, 6.0, ((0, 16), (1, 8)))
    expert_ids_keys = jax.random.split(jax.random.fold_in(own_keys[1], 1), TOKENS // TOK_DEV)
    expert_ids_turns = jax.random.permutation(jax.random.fold_in(own_keys[1], 3), TOKENS // TOK_DEV)
    expert_ids = jax.vmap(lambda own, number: deal_out(jax.random.fold_in(own_keys[1], 2), own, number, TOK_DEV, EXPERTS, TOPK, SLOT, 2))(expert_ids_keys, expert_ids_turns).reshape((TOKENS, TOPK))
    gate_weight = jnp.clip(0.049804688 + 0.24902344 * jax.random.uniform(own_keys[2], (TOKENS, TOPK), jnp.float32) ** block_scale(own_keys[2], (TOKENS, TOPK), ((0, 16),), -0.2, 0.2), 0.049804688, 0.29882812).astype(jnp.bfloat16)
    w_gate = centred(keys[3], (EXPERTS, D, FF), D ** -0.5, 0.09375, ((0, 16), (1, 8)))
    w_up = centred(keys[4], (EXPERTS, D, FF), D ** -0.5, 0.09375, ((0, 16), (1, 8)))
    w_down = centred(keys[5], (EXPERTS, FF, D), FF ** -0.5, 0.21875, ((0, 16), (2, 8)))
    query = draw_query(jax.random.fold_in(jax.random.fold_in(keys[10], part), 71), part)
    cache_k = draw_cache_k(jax.random.fold_in(jax.random.fold_in(keys[10], part), 71), part)
    cache_v = centred(own_keys[8], (SEQS, CTX, KV_HEADS, HEAD_DIM), 1.0, 6.0, ((0, 128),))
    lengths = draw_lengths(jax.random.fold_in(jax.random.fold_in(keys[10], part), 71), part)
    return {"tokens": tokens, "expert_ids": expert_ids, "gate_weight": gate_weight, "w_gate": w_gate, "w_up": w_up, "w_down": w_down, "query": query, "cache_k": cache_k, "cache_v": cache_v, "lengths": lengths}


def one_expert(operands):
    expert_rows, gate_mat, up_mat, down_mat = operands
    blocked = expert_rows.astype(jnp.float32).reshape(CAPACITY, N_EXPERT, FEAT_DEV)
    both_mats = jnp.concatenate([gate_mat, up_mat], axis=1).astype(jnp.float32).reshape(N_EXPERT, FEAT_DEV, 2 * FF)
    partials = jnp.einsum("rbd,bdf->brf", blocked, both_mats)
    rounded = lax.optimization_barrier(partials.astype(jnp.bfloat16))
    both_sums = jnp.sum(rounded.astype(jnp.float32), axis=0)
    hidden = (jax.nn.silu(both_sums[:, :FF]) * both_sums[:, FF:]).astype(jnp.bfloat16)
    return jnp.dot(hidden, down_mat, preferred_element_type=jnp.float32).astype(jnp.bfloat16)


def reference(tokens, expert_ids, gate_weight, w_gate, w_up, w_down, query, cache_k, cache_v, lengths):
    total_rows = tokens.shape[0]
    experts = w_gate.shape[0]
    wanted = jnp.arange(experts, dtype=jnp.int32)
    member = jnp.any(expert_ids[:, :, None] == wanted[None, None, :], axis=1).astype(jnp.int32)
    position = jnp.cumsum(member, axis=0, dtype=jnp.int32) - member
    taken = (member > 0) & (position < CAPACITY)
    target = jnp.where(taken, wanted[None, :] * CAPACITY + position, experts * CAPACITY)
    owners = jnp.broadcast_to(jnp.arange(total_rows, dtype=jnp.int32)[:, None], (total_rows, experts))
    token_index = jnp.full((experts * CAPACITY,), total_rows, jnp.int32).at[target.reshape(-1)].set(owners.reshape(-1), mode="drop")
    padded = jnp.concatenate([tokens, jnp.zeros((1, D), tokens.dtype)], axis=0)
    packed = padded[token_index].reshape(experts, CAPACITY, D)
    results = lax.map(one_expert, (packed, w_gate, w_up, w_down))
    results = lax.optimization_barrier(results)
    place_of = jnp.take_along_axis(position, expert_ids, axis=1)
    keep_mask = place_of < CAPACITY
    flat_index = jnp.where(keep_mask, expert_ids * CAPACITY + place_of, 0)
    picked = results.reshape(experts * CAPACITY, D)[flat_index]
    factor = jnp.where(keep_mask, gate_weight.astype(jnp.float32), 0.0)
    moe_out = jnp.sum(factor[:, :, None] * picked.astype(jnp.float32), axis=1).astype(jnp.bfloat16)

    seq_count = query.shape[0]
    grouped = query.astype(jnp.float32).reshape(seq_count, KV_HEADS, Q_HEADS // KV_HEADS, HEAD_DIM)
    scores = jnp.einsum("skgd,slkd->skgl", grouped, cache_k.astype(jnp.float32)) * (HEAD_DIM ** -0.5)
    live_mask = jnp.arange(CTX, dtype=jnp.int32)[None, None, None, :] < lengths[:, None, None, None]
    masked = jnp.where(live_mask, scores, -jnp.inf)
    row_peak = jnp.max(masked, axis=3, keepdims=True)
    weighted = jnp.exp(masked - row_peak)
    denominator = jnp.sum(weighted, axis=3, keepdims=True)
    prob_bf = lax.optimization_barrier((weighted / denominator).astype(jnp.bfloat16))
    attended = jnp.einsum("skgl,slkd->skgd", prob_bf.astype(jnp.float32), cache_v.astype(jnp.float32))
    attn_out = attended.reshape(seq_count, Q_HEADS * HEAD_DIM).astype(jnp.bfloat16)
    return (moe_out, attn_out)
```

```python
import jax
import jax.numpy as jnp
from jax import lax
from jax.sharding import PartitionSpec as P


def grouped_attention(query, cache_k, cache_v, lengths):
    seq_count, head_total, head_size = query.shape
    context = cache_k.shape[1]
    kv_count = cache_k.shape[2]
    grouped = query.reshape(seq_count, kv_count, head_total // kv_count, head_size)
    scores = jnp.einsum(
        "skgd,slkd->skgl", grouped, cache_k, preferred_element_type=jnp.float32
    ) * head_size ** (-0.5)
    live_mask = (
        lax.broadcasted_iota(jnp.int32, (seq_count, 1, 1, context), 3)
        < lengths[:, None, None, None]
    )
    masked = jnp.where(live_mask, scores, -jnp.inf)
    row_peak = jnp.max(masked, axis=3, keepdims=True)
    weighted = jnp.exp(masked - row_peak)
    denominator = jnp.sum(weighted, axis=3, keepdims=True)
    prob_bf = (weighted / denominator).astype(jnp.bfloat16)
    attended = jnp.einsum("skgl,slkd->skgd", prob_bf, cache_v, preferred_element_type=jnp.float32)
    return attended.reshape(seq_count, head_total * head_size).astype(jnp.bfloat16)


def body(tokens, expert_ids, gate_weight, w_gate, w_up, w_down, query, cache_k, cache_v, lengths):
    tok_rows, feat_width = tokens.shape
    top_count = expert_ids.shape[1]
    local_experts = w_gate.shape[0]
    ffn_width = w_gate.shape[2]
    attn_count = lax.axis_size("attn")
    capacity = tok_rows * top_count // local_experts
    extra = tok_rows * top_count // feat_width
    block = jnp.concatenate(
        [
            tokens,
            expert_ids.astype(jnp.bfloat16).reshape(extra, feat_width),
            gate_weight.reshape(extra, feat_width),
        ],
        axis=0,
    )
    whole = lax.all_gather(block, "attn", axis=0, tiled=False)
    whole_tokens = whole[:, :tok_rows].reshape(attn_count * tok_rows, feat_width)
    whole_ids = whole[:, tok_rows : tok_rows + extra].reshape(attn_count * tok_rows, top_count)
    whole_gates = whole[:, tok_rows + extra :].reshape(attn_count * tok_rows, top_count)
    mine = lax.axis_index("attn") * local_experts + jnp.arange(local_experts, dtype=jnp.int32)
    equal = whole_ids.astype(jnp.int32)[:, :, None] == mine[None, None, :]
    member = jnp.any(equal, axis=1).astype(jnp.int32)
    gates = jnp.sum(jnp.where(equal, whole_gates.astype(jnp.float32)[:, :, None], 0.0), axis=1)
    place = jnp.where(member > 0, jnp.cumsum(member, axis=0, dtype=jnp.int32) - member, -1)
    slots = jnp.arange(capacity, dtype=jnp.int32)
    pick = (place.T[:, None, :] == slots[None, :, None]).astype(jnp.bfloat16)
    packed = jnp.einsum("jrt,td->jrd", pick, whole_tokens, preferred_element_type=jnp.float32).astype(
        jnp.bfloat16
    )
    gate_part = jnp.einsum("jrd,jdf->jrf", packed, w_gate, preferred_element_type=jnp.float32)
    up_part = jnp.einsum("jrd,jdf->jrf", packed, w_up, preferred_element_type=jnp.float32)
    both_parts = jnp.concatenate([gate_part, up_part], axis=2)
    row_sums = lax.psum_scatter(
        both_parts.astype(jnp.bfloat16), "expert", scatter_dimension=1, tiled=True
    ).astype(jnp.float32)
    hidden_share = (jax.nn.silu(row_sums[:, :, :ffn_width]) * row_sums[:, :, ffn_width:]).astype(
        jnp.bfloat16
    )
    hidden = lax.all_gather(hidden_share, "expert", axis=1, tiled=True)
    results = jnp.einsum("jrf,jfd->jrd", hidden, w_down, preferred_element_type=jnp.float32).astype(
        jnp.bfloat16
    )
    weigh = jnp.where(place[:, :, None] == slots[None, None, :], gates[:, :, None], 0.0).astype(
        jnp.bfloat16
    )
    partial = jnp.einsum("tjr,jrd->td", weigh, results, preferred_element_type=jnp.float32)
    moe_out = lax.psum_scatter(
        partial.astype(jnp.bfloat16), "attn", scatter_dimension=0, tiled=True
    )
    attn_out = grouped_attention(query, cache_k, cache_v, lengths)
    return (moe_out, attn_out)


def solution(mesh):
    return jax.shard_map(
        body,
        mesh=mesh,
        in_specs=(
            P(("groups", "attn"), "expert"),
            P(("groups", "attn"), None),
            P(("groups", "attn"), None),
            P("attn", "expert", None),
            P("attn", "expert", None),
            P("attn", None, "expert"),
            P(("groups", "attn", "expert"), None, None),
            P(("groups", "attn", "expert"), None, None, None),
            P(("groups", "attn", "expert"), None, None, None),
            P(("groups", "attn", "expert")),
        ),
        out_specs=(P(("groups", "attn"), "expert"), P(("groups", "attn", "expert"), None)),
        check_vma=False,
    )
```

```python
import functools

import jax
import jax.numpy as jnp
from jax import lax
from jax.experimental import pallas as pl
from jax.experimental.pallas import tpu as pltpu
from jax.sharding import PartitionSpec as P

MESH = pl.DeviceIdType.MESH
BF16 = jnp.bfloat16
F32 = jnp.float32
CORES = 2


def dot(a, b):
    return jnp.dot(a, b, preferred_element_type=F32)


def kernel(
    ny, nx, kv_heads,
    ids_ref, gates_ref, tok_ref, len_ref, q_ref, wg_hbm, wu_hbm, wd_hbm, k_hbm, v_hbm,
    moe_ref, attn_ref,
    wgu, wd, kbuf, vbuf, tok_all, info_all, memb_s, gate_s, pos_s, pos_t, gate_t, acc, part, rs_buf,
    hid, out_all, weigh, comb, d2_send, d2_recv, y_send, y_recv,
    load_sem, inf_s, inf_r, infd_s, infd_r, ag_s, ag_r, agd_s, agd_r, rs_s, rs_r, hx_s, hx_r,
    rd_s, rd_r, ry_s, ry_r,
):
    experts, feat, ff = wg_hbm.shape
    rows = tok_ref.shape[0]
    cap = acc.shape[1]
    share = cap // nx
    hy, hx = ny // 2, nx // 2
    blocks = ny * CORES
    ai, xi = lax.axis_index("attn"), lax.axis_index("expert")
    y, c = lax.div(ai, CORES), lax.rem(ai, CORES)

    def ring(i, n):
        return lax.rem(i + n, n)

    def at_y(i):
        return {"attn": ring(i, ny) * CORES + c}

    partner = {"attn": y * CORES + (1 - c)}
    y_dev = (at_y(y + 1), at_y(y - 1))
    x_dev = ({"expert": ring(xi + 1, nx)}, {"expert": ring(xi - 1, nx)})
    sign = (1, -1)
    sent = []

    def send(src, dst, ss, rs, dev):
        copy = pltpu.make_async_remote_copy(
            src_ref=src, dst_ref=dst, send_sem=ss, recv_sem=rs, device_id=dev, device_id_type=MESH
        )
        copy.start()
        sent.append(copy)
        return copy

    loads = [
        pltpu.make_async_copy(k_hbm, kbuf, load_sem.at[0]),
        pltpu.make_async_copy(v_hbm, vbuf, load_sem.at[1]),
        pltpu.make_async_copy(wg_hbm, wgu.at[:, :, pl.ds(0, ff)], load_sem.at[2]),
        pltpu.make_async_copy(wu_hbm, wgu.at[:, :, pl.ds(ff, ff)], load_sem.at[3]),
        pltpu.make_async_copy(wd_hbm, wd, load_sem.at[4]),
    ]
    for load in loads:
        load.start()
    info = jnp.concatenate([ids_ref[...].astype(F32), gates_ref[...].astype(F32)], axis=0).astype(BF16)
    info_all[y, c] = info
    tok_all[y, c] = tok_ref[...]

    barrier = pltpu.get_barrier_semaphore()
    peers = [at_y(y + k) for k in range(1, ny)] + [partner, x_dev[0], x_dev[1]]
    for dev in peers:
        pl.semaphore_signal(barrier, inc=1, device_id=dev, device_id_type=MESH)
    pl.semaphore_wait(barrier, len(peers))

    info_copy = {
        k: send(info_all.at[y, c], info_all.at[y, c], inf_s.at[k - 1], inf_r.at[k - 1], at_y(y + k))
        for k in range(1, ny)
    }
    info_pair = {0: send(info_all.at[y, c], info_all.at[y, c], infd_s.at[0], infd_r.at[0], partner)}
    half = rows // 2

    def tok_view(piece, yo):
        return tok_all.at[yo, c, pl.ds(piece * half, half)]

    def last_piece(d):
        return d

    ag, pair = {}, {}

    def ag_send(piece, d, s):
        yo = ring(y - sign[d] * (s - 1), ny)
        src = tok_ref.at[pl.ds(piece * half, half)] if s == 1 else tok_view(piece, yo)
        ag[piece, d, s] = send(
            src, tok_view(piece, yo), ag_s.at[piece, d, s - 1], ag_r.at[piece, d, s - 1], y_dev[d]
        )

    def pair_send(piece, d, s):
        yo = ring(y - sign[d] * s, ny)
        slot = 0 if s == 0 else 1 + d * hy + s - 1
        src = tok_ref.at[pl.ds(piece * half, half)] if s == 0 else tok_view(piece, yo)
        pair[piece, d, s] = send(
            src, tok_view(piece, yo), agd_s.at[piece, slot], agd_r.at[piece, slot], partner
        )

    for piece in range(2):
        for d in range(2):
            ag_send(piece, d, 1)
    for piece in range(2):
        pair_send(piece, 0, 0)

    def ag_step(s):
        for piece in range(2):
            for d in range(2):
                if s == hy and piece != last_piece(d):
                    continue
                ag[piece, d, s].wait_recv()
                if s + 1 < hy or (s + 1 == hy and piece == last_piece(d)):
                    ag_send(piece, d, s + 1)
                pair_send(piece, d, s)

    def attention(i):
        heads, size = q_ref.shape[1:]
        keys = kbuf.shape[1]
        group = heads // kv_heads
        scores = lax.dot_general(
            q_ref[i], kbuf[i], (((1,), (1,)), ((), ())), preferred_element_type=F32
        ) * size ** (-0.5)
        col = lax.broadcasted_iota(jnp.int32, (heads, keys), 1)
        head = lax.broadcasted_iota(jnp.int32, (heads, keys), 0)
        live = (lax.rem(col, kv_heads) == lax.div(head, group)) & (
            col < len_ref[i] * kv_heads
        )
        masked = jnp.where(live, scores, -jnp.inf)
        weighted = jnp.exp(masked - jnp.max(masked, axis=1, keepdims=True))
        total = jnp.sum(weighted, axis=1, keepdims=True)
        prob = (weighted * (1.0 / total)).astype(BF16)
        attn_ref[i] = dot(prob, vbuf[i]).astype(BF16)

    loads[0].wait()
    loads[1].wait()
    attention(0)
    ag_step(1)
    for k in range(1, ny):
        info_copy[k].wait_recv()
        yo = ring(y - k, ny)
        info_pair[k] = send(
            info_all.at[yo, c], info_all.at[yo, c], infd_s.at[k], infd_r.at[k], partner
        )
    for i in range(1, q_ref.shape[0]):
        attention(i)
    ag_step(2)

    for k in range(ny):
        info_pair[k].wait_recv()
    top = ids_ref.shape[0]
    first = ai * experts
    for b in range(blocks):
        both = info_all[b // CORES, b % CORES].astype(F32)
        for e in range(experts):
            equal = both[:top] == (first + e).astype(F32)
            row = e * blocks + b
            memb_s[row : row + 1, :] = jnp.sum(jnp.where(equal, 1.0, 0.0), axis=0, keepdims=True)
            gate_s[row : row + 1, :] = jnp.sum(jnp.where(equal, both[top:], 0.0), axis=0, keepdims=True)
    lines = experts * blocks
    member = memb_s[...]
    iota0 = lax.broadcasted_iota(jnp.int32, (rows, rows), 0)
    iota1 = lax.broadcasted_iota(jnp.int32, (rows, rows), 1)
    before = dot(member.astype(BF16), jnp.where(iota0 < iota1, 1.0, 0.0).astype(BF16))
    counts = dot(member.astype(BF16), jnp.ones((rows, rows), BF16))
    line0 = lax.broadcasted_iota(jnp.int32, (lines, lines), 0)
    line1 = lax.broadcasted_iota(jnp.int32, (lines, lines), 1)
    earlier = (lax.div(line0, blocks) == lax.div(line1, blocks)) & (line1 < line0)
    offset = dot(jnp.where(earlier, 1.0, 0.0).astype(BF16), counts.astype(BF16))
    place = jnp.where(member > 0.5, before + offset, -1.0)
    pos_s[...] = place
    pad = jnp.zeros((rows - lines, rows), F32)
    pos_t[...] = jnp.concatenate([place, pad], axis=0).T
    gate_t[...] = jnp.concatenate([gate_s[...], pad], axis=0).T

    slot_row = lax.broadcasted_iota(jnp.int32, (cap, rows), 0).astype(F32)

    def dispatch(e, yc):
        picks = []
        for cc in range(CORES):
            line = pos_s[pl.ds(e * blocks + yc * CORES + cc, 1), :]
            picks.append(jnp.where(line == slot_row, 1.0, 0.0))
        pick = jnp.concatenate(picks, axis=1).astype(BF16)
        return dot(pick, tok_all[yc].reshape(CORES * rows, feat))

    def pair_wait(s):
        for (piece, d, at), copy in pair.items():
            if at == s:
                copy.wait_recv()

    pair_wait(0)
    for e in range(experts):
        acc[e] = dispatch(e, y)

    def dispatch_step(s):
        pair_wait(s)
        for d in range(2):
            for e in range(experts):
                acc[e] += dispatch(e, ring(y - sign[d] * s, ny))

    dispatch_step(1)
    for s in range(3, hy + 1):
        ag_step(s)
        dispatch_step(s - 1)
    pair_wait(hy)

    loads[2].wait()
    loads[3].wait()
    rs = {}
    half_share = share // 2

    def rs_send(e, d, s):
        dest = ring(xi + sign[d] * (hx + 1 - s), nx)
        if s == 1:
            at = pl.ds(d * half_share, half_share)
            src, dst = part.at[e, dest, at], rs_buf.at[d, 0, e, at]
        else:
            src, dst = rs_buf.at[d, s - 2, e], rs_buf.at[d, s - 1, e]
        rs[e, d, s] = send(src, dst, rs_s.at[e, d, s - 1], rs_r.at[e, d, s - 1], x_dev[d])

    wide = 2 * ff
    step_cols = wide // 3
    for e in range(experts):
        packed = (acc[e] + dispatch(e, ring(y + hy, ny))).astype(BF16)
        for n in range(3):
            at = pl.ds(n * step_cols, step_cols)
            part[e, :, :, at] = (
                dot(packed, wgu[e, :, at]).astype(BF16).reshape(nx, share, step_cols)
            )
        for d in range(2):
            rs_send(e, d, 1)

    slot_col = lax.broadcasted_iota(jnp.int32, (rows, cap), 1).astype(F32)

    def weigh_block(b):
        for e in range(experts):
            line = e * blocks + b
            at_col = pos_t[:, line : line + 1]
            gate_col = gate_t[:, line : line + 1]
            weigh[b // CORES, b % CORES, :, e * cap : (e + 1) * cap] = jnp.where(
                at_col == slot_col, gate_col, 0.0
            ).astype(BF16)

    todo = list(range(blocks))
    for s in range(1, hx):
        for e in range(experts):
            for d in range(2):
                rs[e, d, s].wait_recv()
                dest = ring(xi + sign[d] * (hx - s), nx)
                if s == 1:
                    got, new = pl.ds(d * half_share, half_share), pl.ds((1 - d) * half_share, half_share)
                    rs_buf[d, 0, e, got] = (
                        rs_buf[d, 0, e, got].astype(F32) + part[e, dest, got].astype(F32)
                    ).astype(BF16)
                    rs_buf[d, 0, e, new] = part[e, dest, new]
                else:
                    rs_buf[d, s - 1, e] = (
                        rs_buf[d, s - 1, e].astype(F32) + part[e, dest].astype(F32)
                    ).astype(BF16)
                rs_send(e, d, s + 1)
            for _ in range(2):
                if todo:
                    weigh_block(todo.pop(0))

    hd = {}

    def hid_send(e, d, s):
        xo = ring(xi - sign[d] * (s - 1), nx)
        view = hid.at[e, xo]
        if s == hx:
            view = hid.at[e, xo, pl.ds(d * half_share, half_share)]
        hd[e, d, s] = send(view, view, hx_s.at[e, d, s - 1], hx_r.at[e, d, s - 1], x_dev[d])

    for e in range(experts):
        for d in range(2):
            rs[e, d, hx].wait_recv()
        total = part[e, xi].astype(F32) + rs_buf[0, hx - 1, e].astype(F32) + rs_buf[1, hx - 1, e].astype(F32)
        gate = total[:, :ff]
        hid[e, xi] = (gate / (1.0 + jnp.exp(-gate)) * total[:, ff:]).astype(BF16)
        for d in range(2):
            hid_send(e, d, 1)
    for s in range(1, hx):
        for e in range(experts):
            for d in range(2):
                hd[e, d, s].wait_recv()
                hid_send(e, d, s + 1)
    loads[4].wait()
    for e in range(experts):
        for d in range(2):
            hd[e, d, hx].wait_recv()
        out_all[e * cap : (e + 1) * cap, :] = dot(hid[e].reshape(cap, ff), wd[e]).astype(BF16)

    def slot_of(d, k):
        return 0 if k == 0 else ny - 1 if k == hy else 2 * k - 1 + d

    rd = {}

    def combine(d, k):
        slot = slot_of(d, k)
        yd = ring(y + sign[d] * k, ny)
        d2_send[slot] = dot(weigh[yd, 1 - c], out_all[...]).astype(BF16)
        rd[slot] = send(d2_send.at[slot], d2_recv.at[slot], rd_s.at[slot], rd_r.at[slot], partner)
        comb[slot] = dot(weigh[yd, c], out_all[...])

    def join(d, k):
        slot = slot_of(d, k)
        rd[slot].wait_recv()
        comb[slot] += d2_recv[slot].astype(F32)

    pieces = 4
    tall = rows // pieces
    ry = {}

    def ry_has(p, d, s):
        return s > 1 or (p >= pieces // 2) == (d == 1)

    def ry_step(s):
        for p in range(pieces):
            for d in range(2):
                if not ry_has(p, d, s):
                    continue
                at = pl.ds(p * tall, tall)
                value = comb[slot_of(d, hy + 1 - s), at]
                if s > 1 and ry_has(p, d, s - 1):
                    ry[p, d, s - 1].wait_recv()
                    value = value + y_recv[d, s - 2, at].astype(F32)
                y_send[d, s - 1, at] = value.astype(BF16)
                ry[p, d, s] = send(
                    y_send.at[d, s - 1, at], y_recv.at[d, s - 1, at],
                    ry_s.at[p, d, s - 1], ry_r.at[p, d, s - 1], y_dev[d],
                )

    combine(0, hy)
    for s in range(1, hy + 1):
        k = hy - s
        for d in range(2 if k else 1):
            combine(d, k)
        for d in range(2 if s > 1 else 1):
            join(d, k + 1)
        ry_step(s)
    join(0, 0)
    for p in range(pieces):
        at = pl.ds(p * tall, tall)
        value = comb[0, at]
        for d in range(2):
            ry[p, d, hy].wait_recv()
            value = value + y_recv[d, hy - 1, at].astype(F32)
        moe_ref[at, :] = value.astype(BF16)
    for copy in sent:
        copy.wait_send()


def body(tokens, expert_ids, gate_weight, w_gate, w_up, w_down, query, cache_k, cache_v, lengths):
    rows, feat = tokens.shape
    top = expert_ids.shape[1]
    experts, _, ff = w_gate.shape
    attn, nx = lax.axis_size("attn"), lax.axis_size("expert")
    ny = attn // CORES
    cap = rows * top // experts
    share = cap // nx
    seqs, heads, size = query.shape
    context, kv_heads = cache_k.shape[1:3]
    keys = context * kv_heads
    lines = experts * attn
    hy, hx = ny // 2, nx // 2
    vmem = pltpu.VMEM
    sem = pltpu.SemaphoreType.DMA
    in_vmem = pl.BlockSpec(memory_space=vmem)
    in_hbm = pl.BlockSpec(memory_space=pl.ANY)
    moe, attended = pl.pallas_call(
        functools.partial(kernel, ny, nx, kv_heads),
        out_shape=(
            jax.ShapeDtypeStruct((rows, feat), BF16),
            jax.ShapeDtypeStruct((seqs, heads, size), BF16),
        ),
        in_specs=[in_vmem, in_vmem, in_vmem, pl.BlockSpec(memory_space=pltpu.SMEM), in_vmem] + [in_hbm] * 5,
        out_specs=(in_vmem, in_vmem),
        scratch_shapes=[
            vmem((experts, feat, 2 * ff), BF16),
            vmem((experts, ff, feat), BF16),
            vmem((seqs, keys, size), BF16),
            vmem((seqs, keys, size), BF16),
            vmem((ny, CORES, rows, feat), BF16),
            vmem((ny, CORES, 2 * top, rows), BF16),
            vmem((lines, rows), F32),
            vmem((lines, rows), F32),
            vmem((lines, rows), F32),
            vmem((rows, rows), F32),
            vmem((rows, rows), F32),
            vmem((experts, cap, feat), F32),
            vmem((experts, nx, share, 2 * ff), BF16),
            vmem((2, hx, experts, share, 2 * ff), BF16),
            vmem((experts, nx, share, ff), BF16),
            vmem((experts * cap, feat), BF16),
            vmem((ny, CORES, rows, experts * cap), BF16),
            vmem((ny, rows, feat), F32),
            vmem((ny, rows, feat), BF16),
            vmem((ny, rows, feat), BF16),
            vmem((2, hy, rows, feat), BF16),
            vmem((2, hy, rows, feat), BF16),
            sem((5,)),
            sem((ny - 1,)), sem((ny - 1,)), sem((ny,)), sem((ny,)),
            sem((2, 2, hy)), sem((2, 2, hy)), sem((2, 2 * hy + 1)), sem((2, 2 * hy + 1)),
            sem((experts, 2, hx)), sem((experts, 2, hx)),
            sem((experts, 2, hx)), sem((experts, 2, hx)),
            sem((ny,)), sem((ny,)),
            sem((4, 2, hy)), sem((4, 2, hy)),
        ],
        compiler_params=pltpu.CompilerParams(
            collective_id=0, has_side_effects=True, vmem_limit_bytes=56 * 1024 * 1024
        ),
        name="experts_and_attention",
    )(
        expert_ids.T, gate_weight.T, tokens, lengths, query, w_gate, w_up, w_down,
        cache_k.reshape(seqs, keys, size), cache_v.reshape(seqs, keys, size),
    )
    return (moe, attended.reshape(seqs, heads * size))


def solution(mesh):
    return jax.shard_map(
        body,
        mesh=mesh,
        in_specs=(
            P(("groups", "attn"), "expert"),
            P(("groups", "attn"), None),
            P(("groups", "attn"), None),
            P("attn", "expert", None),
            P("attn", "expert", None),
            P("attn", None, "expert"),
            P(("groups", "attn", "expert"), None, None),
            P(("groups", "attn", "expert"), None, None, None),
            P(("groups", "attn", "expert"), None, None, None),
            P(("groups", "attn", "expert")),
        ),
        out_specs=(P(("groups", "attn"), "expert"), P(("groups", "attn", "expert"), None)),
        check_vma=False,
    )
```

```python
import functools

import jax
import jax.numpy as jnp
from jax import lax
from jax.experimental import pallas as pl
from jax.experimental.pallas import tpu as pltpu
from jax.sharding import PartitionSpec as P

MESH = pl.DeviceIdType.MESH
BF16 = jnp.bfloat16
F32 = jnp.float32
CORES = 2


def dot(a, b):
    return jnp.dot(a, b, preferred_element_type=F32)


def kernel(
    ny, nx, kv_heads,
    ids_hbm, gates_hbm, tok_hbm, len_hbm, q_hbm, wg_hbm, wu_hbm, wd_hbm, k_hbm, v_hbm,
    moe_ref, attn_ref,
    ids_ref, gates_ref, tok_ref, len_ref, q_ref,
    wgu, wd, kbuf, vbuf, tok_all, info_all, memb_s, gate_s, pos_s, pos_t, gate_t, acc, part, rs_buf,
    hid, out_all, weigh, comb, d2_send, d2_recv, y_send, y_recv, moe_s, attn_s,
    load_sem, w_sem, wd_sem, kv_sem, store_sem, out_sem, inf_r, infd_r, ag_r, agd_r, rs_r, hx_r, rd_r, ry_r,
):
    experts, feat, ff = wg_hbm.shape
    rows = tok_ref.shape[0]
    cap = acc.shape[1]
    share = cap // nx
    hy, hx = ny // 2, nx // 2
    blocks = ny * CORES
    seqs = q_hbm.shape[0]
    ai, xi = lax.axis_index("attn"), lax.axis_index("expert")
    y, c = lax.div(ai, CORES), lax.rem(ai, CORES)

    def ring(i, n):
        return lax.rem(i + n, n)

    def at_y(i):
        return {"attn": ring(i, ny) * CORES + c}

    partner = {"attn": y * CORES + (1 - c)}
    y_dev = (at_y(y + 1), at_y(y - 1))
    x_dev = ({"expert": ring(xi + 1, nx)}, {"expert": ring(xi - 1, nx)})
    sign = (1, -1)

    barrier = pltpu.get_barrier_semaphore()
    peers = [*y_dev, partner, *x_dev]
    for dev in peers:
        pl.semaphore_signal(barrier, inc=1, device_id=dev, device_id_type=MESH)

    def send(src, dst, kind, recv_sem, dev):
        copy = pltpu.make_async_remote_copy(
            src_ref=src, dst_ref=dst, send_sem=out_sem.at[kind], recv_sem=recv_sem,
            device_id=dev, device_id_type=MESH,
        )
        copy.start()
        return copy

    def wait_bytes(sem, ref):
        pltpu.make_async_copy(ref, ref, sem).wait()

    def load(src, dst, sem):
        copy = pltpu.make_async_copy(src, dst, sem)
        copy.start()
        return copy

    small = [
        load(tok_hbm, tok_ref, load_sem.at[0]),
        load(ids_hbm, ids_ref, load_sem.at[1]),
        load(gates_hbm, gates_ref, load_sem.at[2]),
    ]
    for copy in small[1:]:
        copy.wait()
    info = jnp.concatenate([ids_ref[...].astype(F32), gates_ref[...].astype(F32)], axis=0).astype(BF16)
    info_all[y, c] = info
    small[0].wait()
    pl.semaphore_wait(barrier, len(peers))

    INFO, PAIR_INFO, AG, PAIR, RS, HD, RD, RY = range(8)
    pieces = 4
    tall = rows // pieces

    def goes(p, d):
        return (p >= pieces // 2) == (d == 1)

    def piece_at(p):
        return pl.ds(p * tall, tall)

    def tok_view(p, yo):
        return tok_all.at[yo, c, piece_at(p)]

    ag, inf = {}, {}

    def ag_send(p, d, s):
        yo = ring(y - sign[d] * (s - 1), ny)
        src = tok_ref.at[piece_at(p)] if s == 1 else tok_view(p, yo)
        ag[p, d, s] = send(src, tok_view(p, yo), AG, ag_r.at[p, d, s - 1], y_dev[d])

    def pair_send(p, d, s):
        yo = ring(y - sign[d] * s, ny)
        src = tok_ref.at[piece_at(p)] if s == 0 else tok_view(p, yo)
        send(src, tok_view(p, yo), PAIR, agd_r.at[s], partner)

    def info_send(d, s):
        view = info_all.at[ring(y - sign[d] * (s - 1), ny), c]
        inf[d, s] = send(view, view, INFO, inf_r.at[d, s - 1], y_dev[d])

    def info_pair(d, s):
        view = info_all.at[ring(y - sign[d] * s, ny), c]
        send(view, view, PAIR_INFO, infd_r.at[0], partner)

    def info_step(s):
        for d in range(2 if s < hy else 1):
            inf[d, s].wait_recv()
            if s + 1 < hy or (s + 1 == hy and d == 0):
                info_send(d, s + 1)
            info_pair(d, s)

    def ag_step(s, p):
        for d in range(2):
            if s == hy and not goes(p, d):
                continue
            ag[p, d, s].wait_recv()
            if s + 1 < hy or (s + 1 == hy and goes(p, d)):
                ag_send(p, d, s + 1)
            pair_send(p, d, s)

    turn = (0, 2, 1, 3)
    for d in range(2):
        info_send(d, 1)
    for p in turn:
        for d in range(2):
            ag_send(p, d, 1)
    info_pair(0, 0)
    for p in range(pieces):
        pair_send(p, 0, 0)
    tok_all[y, c] = tok_ref[...]

    weights = {}

    def load_weights(e):
        weights[e] = (
            load(wg_hbm.at[e], wgu.at[e, :, pl.ds(0, ff)], w_sem.at[0, e]),
            load(wu_hbm.at[e], wgu.at[e, :, pl.ds(ff, ff)], w_sem.at[1, e]),
        )

    def places():
        wait_bytes(infd_r.at[0], info_all.at[:, 0])
        top = ids_ref.shape[0]
        first = ai * experts
        for b in range(blocks):
            both = info_all[b // CORES, b % CORES].astype(F32)
            for e in range(experts):
                equal = both[:top] == (first + e).astype(F32)
                row = e * blocks + b
                memb_s[row : row + 1, :] = jnp.sum(jnp.where(equal, 1.0, 0.0), axis=0, keepdims=True)
                gate_s[row : row + 1, :] = jnp.sum(jnp.where(equal, both[top:], 0.0), axis=0, keepdims=True)
        lines = experts * blocks
        member = memb_s[...]
        iota0 = lax.broadcasted_iota(jnp.int32, (rows, rows), 0)
        iota1 = lax.broadcasted_iota(jnp.int32, (rows, rows), 1)
        before = dot(member.astype(BF16), jnp.where(iota0 < iota1, 1.0, 0.0).astype(BF16))
        counts = dot(member.astype(BF16), jnp.ones((rows, rows), BF16))
        line0 = lax.broadcasted_iota(jnp.int32, (lines, lines), 0)
        line1 = lax.broadcasted_iota(jnp.int32, (lines, lines), 1)
        earlier = (lax.div(line0, blocks) == lax.div(line1, blocks)) & (line1 < line0)
        offset = dot(jnp.where(earlier, 1.0, 0.0).astype(BF16), counts.astype(BF16))
        pos_s[...] = jnp.where(member > 0.5, before + offset, -1.0)

    def turned():
        pad = jnp.zeros((rows - experts * blocks, rows), F32)
        pos_t[...] = jnp.concatenate([pos_s[...], pad], axis=0).T
        gate_t[...] = jnp.concatenate([gate_s[...], pad], axis=0).T

    slot_row = lax.broadcasted_iota(jnp.int32, (cap, rows), 0).astype(F32)

    def dispatch(e, yc):
        picks = []
        for cc in range(CORES):
            line = pos_s[pl.ds(e * blocks + yc * CORES + cc, 1), :]
            picks.append(jnp.where(line == slot_row, 1.0, 0.0))
        pick = jnp.concatenate(picks, axis=1).astype(BF16)
        return dot(pick, tok_all[yc].reshape(CORES * rows, feat))

    def pair_wait(s):
        wait_bytes(agd_r.at[s], tok_all.at[0] if 0 < s < hy else tok_all.at[0, 0])

    def gather_in(s, d):
        if d == 0:
            pair_wait(s)
        for e in range(experts):
            new = dispatch(e, ring(y - sign[d] * s, ny))
            acc[e] = new if s == 0 else acc[e] + new

    info_step(1)
    for n, p in enumerate(turn):
        ag_step(1, p)
    info_step(2)
    for n, p in enumerate(turn):
        ag_step(2, p)
        load_weights(n)
        if n == 1:
            info_step(3)
    ag_step(3, turn[0])
    info_step(4)
    ag_step(3, turn[1])
    places()
    ag_step(3, turn[2])
    gather_in(0, 0)
    ag_step(3, turn[3])
    gather_in(1, 0)
    gather_in(1, 1)
    ag_step(4, turn[0])
    ag_step(4, turn[1])
    gather_in(2, 0)
    ag_step(4, turn[2])
    ag_step(4, turn[3])
    gather_in(2, 1)
    gather_in(3, 0)
    gather_in(3, 1)
    pair_wait(hy)

    rs = {}
    half_share = share // 2

    def rs_send(e, d, s):
        dest = ring(xi + sign[d] * (hx + 1 - s), nx)
        if s == 1:
            at = pl.ds(d * half_share, half_share)
            src, dst = part.at[e, dest, at], rs_buf.at[d, 0, e, at]
        else:
            src, dst = rs_buf.at[d, s - 2, e], rs_buf.at[d, s - 1, e]
        rs[e, d, s] = send(src, dst, RS, rs_r.at[e, d, s - 1], x_dev[d])

    wide = 2 * ff
    step_cols = wide // 3
    for e in range(experts):
        packed = (acc[e] + dispatch(e, ring(y + hy, ny))).astype(BF16)
        for copy in weights[e]:
            copy.wait()
        for n in range(3):
            at = pl.ds(n * step_cols, step_cols)
            part[e, :, :, at] = (
                dot(packed, wgu[e, :, at]).astype(BF16).reshape(nx, share, step_cols)
            )
        for d in range(2):
            rs_send(e, d, 1)

    slot_col = lax.broadcasted_iota(jnp.int32, (rows, cap), 1).astype(F32)

    def weigh_block(b):
        for e in range(experts):
            line = e * blocks + b
            at_col = pos_t[:, line : line + 1]
            gate_col = gate_t[:, line : line + 1]
            weigh[b // CORES, b % CORES, :, e * cap : (e + 1) * cap] = jnp.where(
                at_col == slot_col, gate_col, 0.0
            ).astype(BF16)

    attn_in, stores, down_in = {}, [], {}

    def load_attention(i):
        attn_in[i] = [
            load(k_hbm.at[i], kbuf.at[i], kv_sem.at[i, 0]),
            load(v_hbm.at[i], vbuf.at[i], kv_sem.at[i, 1]),
            load(q_hbm.at[i], q_ref.at[i], kv_sem.at[i, 2]),
        ]
        if i == 0:
            attn_in[i].append(load(len_hbm, len_ref, load_sem.at[3]))

    def attend(i):
        for copy in attn_in[i]:
            copy.wait()
        heads, size = q_ref.shape[1:]
        keys = kbuf.shape[1]
        group = heads // kv_heads
        scores = lax.dot_general(
            q_ref[i], kbuf[i], (((1,), (1,)), ((), ())), preferred_element_type=F32
        ) * size ** (-0.5)
        col = lax.broadcasted_iota(jnp.int32, (heads, keys), 1)
        head = lax.broadcasted_iota(jnp.int32, (heads, keys), 0)
        live = (lax.rem(col, kv_heads) == lax.div(head, group)) & (col < len_ref[i] * kv_heads)
        masked = jnp.where(live, scores, -jnp.inf)
        weighted = jnp.exp(masked - jnp.max(masked, axis=1, keepdims=True))
        total = jnp.sum(weighted, axis=1, keepdims=True)
        prob = (weighted * (1.0 / total)).astype(BF16)
        attn_s[i] = dot(prob, vbuf[i]).astype(BF16)
        stores.append(load(attn_s.at[i], attn_ref.at[i], store_sem.at[i]))

    def load_down(e):
        down_in[e] = load(wd_hbm.at[e], wd.at[e], wd_sem.at[e])

    def settle_early():
        wait_bytes(out_sem.at[INFO], info_all.at[pl.ds(0, ny - 1), 0])
        wait_bytes(out_sem.at[PAIR_INFO], info_all.at[:, 0])
        wait_bytes(out_sem.at[AG], d2_recv.at[pl.ds(0, ny - 1)])
        wait_bytes(out_sem.at[PAIR], d2_recv)

    def weigh_blocks(b):
        weigh_block(b)
        weigh_block(b + 1)

    todo = [turned] + [functools.partial(load_attention, i) for i in range(seqs)]
    todo += [functools.partial(load_down, e) for e in range(experts)]
    todo += [functools.partial(attend, i) for i in range(seqs)]
    todo += [functools.partial(weigh_blocks, b) for b in range(0, blocks, 2)]
    todo += [settle_early]
    for s in range(1, hx):
        for e in range(experts):
            for d in range(2):
                rs[e, d, s].wait_recv()
                dest = ring(xi + sign[d] * (hx - s), nx)
                if s == 1:
                    got, new = pl.ds(d * half_share, half_share), pl.ds((1 - d) * half_share, half_share)
                    rs_buf[d, 0, e, got] = (
                        rs_buf[d, 0, e, got].astype(F32) + part[e, dest, got].astype(F32)
                    ).astype(BF16)
                    rs_buf[d, 0, e, new] = part[e, dest, new]
                else:
                    rs_buf[d, s - 1, e] = (
                        rs_buf[d, s - 1, e].astype(F32) + part[e, dest].astype(F32)
                    ).astype(BF16)
                rs_send(e, d, s + 1)
            for _ in range(1 if s == 1 else 2):
                if todo:
                    todo.pop(0)()
    for job in todo:
        job()

    hd = {}

    def hid_send(e, d, s):
        xo = ring(xi - sign[d] * (s - 1), nx)
        view = hid.at[e, xo]
        if s == hx:
            view = hid.at[e, xo, pl.ds(d * half_share, half_share)]
        hd[e, d, s] = send(view, view, HD, hx_r.at[e, d, s - 1], x_dev[d])

    for e in range(experts):
        for d in range(2):
            rs[e, d, hx].wait_recv()
        total = part[e, xi].astype(F32) + rs_buf[0, hx - 1, e].astype(F32) + rs_buf[1, hx - 1, e].astype(F32)
        gate = total[:, :ff]
        hid[e, xi] = (gate / (1.0 + jnp.exp(-gate)) * total[:, ff:]).astype(BF16)
        for d in range(2):
            hid_send(e, d, 1)
    for s in range(1, hx):
        for e in range(experts):
            for d in range(2):
                hd[e, d, s].wait_recv()
                hid_send(e, d, s + 1)
    wait_bytes(out_sem.at[RS], part.at[:, pl.ds(0, nx - 1)])
    for e in range(experts):
        down_in[e].wait()
        for d in range(2):
            hd[e, d, hx].wait_recv()
        out_all[e * cap : (e + 1) * cap, :] = dot(hid[e].reshape(cap, ff), wd[e]).astype(BF16)

    def slot_of(d, k):
        return 0 if k == 0 else ny - 1 if k == hy else 2 * k - 1 + d

    rd, ry = {}, {}

    def combine(d, k):
        slot = slot_of(d, k)
        yd = ring(y + sign[d] * k, ny)
        both = dot(weigh[yd].reshape(CORES * rows, experts * cap), out_all[...]).reshape(CORES, rows, feat)
        d2_send[slot] = both.astype(BF16)
        rd[slot] = send(d2_send.at[slot, 1 - c], d2_recv.at[slot], RD, rd_r.at[slot], partner)
        comb[slot] = both

    def join(d, k):
        slot = slot_of(d, k)
        rd[slot].wait_recv()
        comb[slot, c] += d2_recv[slot].astype(F32)

    def ry_step(s, long):
        for p in turn:
            for d in range(2):
                if goes(p, d) != long:
                    continue
                at = piece_at(p)
                value = comb[slot_of(d, hy + 1 - s), c, at]
                if s > (1 if long else 2):
                    ry[p, d, s - 1].wait_recv()
                    value = value + y_recv[d, s - 2, at].astype(F32)
                y_send[d, s - 1, at] = value.astype(BF16)
                ry[p, d, s] = send(
                    y_send.at[d, s - 1, at], y_recv.at[d, s - 1, at], RY, ry_r.at[p, d, s - 1], y_dev[d]
                )

    def both_ways(job, k):
        for d in range(2 if 0 < k < hy else 1):
            job(d, k)

    both_ways(combine, hy)
    both_ways(combine, hy - 1)
    both_ways(join, hy)
    ry_step(1, True)
    both_ways(combine, hy - 2)
    both_ways(join, hy - 1)
    ry_step(2, False)
    for k in range(hy - 3, -1, -1):
        both_ways(combine, k)
    both_ways(join, hy - 2)
    ry_step(2, True)
    for s in range(3, hy + 1):
        ry_step(s, False)
        if s < hy:
            both_ways(join, hy - s)
        else:
            join(0, 0)
        ry_step(s, True)
    wait_bytes(out_sem.at[HD], hid.at[:, pl.ds(0, nx - 1)])
    wait_bytes(out_sem.at[RD], d2_recv)
    for p in turn:
        at = piece_at(p)
        value = comb[0, c, at]
        for d in range(2):
            ry[p, d, hy].wait_recv()
            value = value + y_recv[d, hy - 1, at].astype(F32)
        moe_s[at, :] = value.astype(BF16)
        stores.append(load(moe_s.at[at], moe_ref.at[at], store_sem.at[len(stores)]))
    wait_bytes(out_sem.at[RY], d2_recv.at[pl.ds(0, ny - 1)])
    for store in stores:
        store.wait()


def body(tokens, expert_ids, gate_weight, w_gate, w_up, w_down, query, cache_k, cache_v, lengths):
    rows, feat = tokens.shape
    top = expert_ids.shape[1]
    experts, _, ff = w_gate.shape
    attn, nx = lax.axis_size("attn"), lax.axis_size("expert")
    ny = attn // CORES
    cap = rows * top // experts
    share = cap // nx
    seqs, heads, size = query.shape
    context, kv_heads = cache_k.shape[1:3]
    keys = context * kv_heads
    lines = experts * attn
    hy, hx = ny // 2, nx // 2
    vmem = pltpu.VMEM
    sem = pltpu.SemaphoreType.DMA
    in_hbm = pl.BlockSpec(memory_space=pl.ANY)
    moe, attended = pl.pallas_call(
        functools.partial(kernel, ny, nx, kv_heads),
        out_shape=(
            jax.ShapeDtypeStruct((rows, feat), BF16),
            jax.ShapeDtypeStruct((seqs, heads, size), BF16),
        ),
        in_specs=[in_hbm] * 10,
        out_specs=(in_hbm, in_hbm),
        scratch_shapes=[
            vmem((top, rows), jnp.int32),
            vmem((top, rows), BF16),
            vmem((rows, feat), BF16),
            pltpu.SMEM((seqs,), jnp.int32),
            vmem((seqs, heads, size), BF16),
            vmem((experts, feat, 2 * ff), BF16),
            vmem((experts, ff, feat), BF16),
            vmem((seqs, keys, size), BF16),
            vmem((seqs, keys, size), BF16),
            vmem((ny, CORES, rows, feat), BF16),
            vmem((ny, CORES, 2 * top, rows), BF16),
            vmem((lines, rows), F32),
            vmem((lines, rows), F32),
            vmem((lines, rows), F32),
            vmem((rows, rows), F32),
            vmem((rows, rows), F32),
            vmem((experts, cap, feat), F32),
            vmem((experts, nx, share, 2 * ff), BF16),
            vmem((2, hx, experts, share, 2 * ff), BF16),
            vmem((experts, nx, share, ff), BF16),
            vmem((experts * cap, feat), BF16),
            vmem((ny, CORES, rows, experts * cap), BF16),
            vmem((ny, CORES, rows, feat), F32),
            vmem((ny, CORES, rows, feat), BF16),
            vmem((ny, rows, feat), BF16),
            vmem((2, hy, rows, feat), BF16),
            vmem((2, hy, rows, feat), BF16),
            vmem((rows, feat), BF16),
            vmem((seqs, heads, size), BF16),
            sem((4,)), sem((2, experts)), sem((experts,)), sem((seqs, 3)), sem((seqs + 4,)), sem((8,)),
            sem((2, hy)), sem((1,)), sem((4, 2, hy)), sem((hy + 1,)),
            sem((experts, 2, hx)), sem((experts, 2, hx)), sem((ny,)), sem((4, 2, hy)),
        ],
        compiler_params=pltpu.CompilerParams(
            collective_id=0, has_side_effects=True, vmem_limit_bytes=56 * 1024 * 1024
        ),
        name="experts_and_attention",
    )(
        expert_ids.T, gate_weight.T, tokens, lengths, query, w_gate, w_up, w_down,
        cache_k.reshape(seqs, keys, size), cache_v.reshape(seqs, keys, size),
    )
    return (moe, attended.reshape(seqs, heads * size))


def solution(mesh):
    return jax.shard_map(
        body,
        mesh=mesh,
        in_specs=(
            P(("groups", "attn"), "expert"),
            P(("groups", "attn"), None),
            P(("groups", "attn"), None),
            P("attn", "expert", None),
            P("attn", "expert", None),
            P("attn", None, "expert"),
            P(("groups", "attn", "expert"), None, None),
            P(("groups", "attn", "expert"), None, None, None),
            P(("groups", "attn", "expert"), None, None, None),
            P(("groups", "attn", "expert")),
        ),
        out_specs=(P(("groups", "attn"), "expert"), P(("groups", "attn", "expert"), None)),
        check_vma=False,
    )
```
